32 devices in a mesh: fsdp: 16 (over z, x, core), tp: 2 (over y).
Axes of the slice: x: 2, y: 2, z: 4, core: 2. Of those that a mesh axis runs over, the one named last changes fastest.
Arguments:
- grad_iterate: bfloat16 [3584, 18432], P('tp', 'fsdp'), may hold values from -0.036828478 to 0.036828478
Outputs:
- update: float32 [3584, 18432], P('tp', 'fsdp')
The draws below stay inside these ranges and needn't reach their ends.
All inputs are finite; a program needn't handle non-finite values.
Results may differ from the reference program's by a relative error of at most 0.0031.
Values may be sent and summed in bfloat16 or wider, within the bound.
A program may use at most 128 MiB of HBM per device.

```python
import math
import jax
import jax.numpy as jnp

R = 3584
C = 18432


def draw_grad_iterate(key, part):
    key_one = jax.random.fold_in(key, 11)
    key_two = jax.random.fold_in(key, 23)
    key_four = jax.random.fold_in(key, 41)
    key_five = jax.random.fold_in(key, 53)
    key_six = jax.random.fold_in(key, 67)
    shared_rank = max(R // 4, 1)
    row_scale = jnp.exp(jax.random.uniform(key_two, (R, 1), jnp.float32, math.log(0.1), 0.0))
    factor_gain = jnp.exp(jax.random.uniform(key_six, (1, shared_rank), jnp.float32, math.log(0.4), math.log(1.6)))
    factor_gain = factor_gain / jnp.sqrt(jnp.mean(factor_gain * factor_gain))
    left_factor = jax.random.normal(key_four, (R, shared_rank), jnp.float32) * factor_gain
    right_factor = jax.random.normal(key_five, (shared_rank, C), jnp.float32)
    shared = jnp.dot(left_factor, right_factor) / math.sqrt(shared_rank)
    noise = jax.random.normal(key_one, (R, C), jnp.float32)
    entries = jnp.clip(0.25 * noise + 0.9 * shared, -3.5, 3.5)
    return (entries * row_scale / math.sqrt(C)).astype(jnp.bfloat16)


def setup_inputs(seed: int = 0) -> dict:
    arg_keys = jax.random.split(jax.random.key(seed), 2)
    return {
        "grad_iterate": draw_grad_iterate(jax.random.fold_in(arg_keys[1], 71), 0),
    }


quintic_one = 3.4445
quintic_three = -4.775
quintic_five = 2.0315

def reference(grad_iterate):
    gram = jnp.dot(grad_iterate, grad_iterate.T, preferred_element_type=jnp.float32)
    gram_low = gram.astype(jnp.bfloat16)
    applied = jnp.dot(gram_low, grad_iterate, preferred_element_type=jnp.float32)
    applied_low = applied.astype(jnp.bfloat16)
    twice_applied = jnp.dot(gram_low, applied_low, preferred_element_type=jnp.float32)
    mixed = quintic_one * grad_iterate.astype(jnp.float32) + quintic_three * applied + quintic_five * twice_applied
    return mixed * math.sqrt(C)
```

```python
import functools
import math

import jax
import jax.numpy as jnp
from jax import lax
from jax.sharding import PartitionSpec as P

C = 18432


quintic_one = 3.4445
quintic_three = -4.775
quintic_five = 2.0315


def rows_by_rows(a, b):
    return lax.dot_general(a, b, (((1,), (1,)), ((), ())), preferred_element_type=jnp.float32)


def matmul(a, b):
    return jnp.dot(a, b, preferred_element_type=jnp.float32)


def general(grad_iterate):
    columns = lax.all_gather(grad_iterate, "tp", axis=0, tiled=True)
    shares = lax.psum_scatter(
        rows_by_rows(columns, grad_iterate), "fsdp", scatter_dimension=0, tiled=True
    )
    gram_cols = lax.all_gather(shares.astype(jnp.bfloat16), "fsdp", axis=0, tiled=True)
    applied = lax.dot_general(
        gram_cols, columns, (((0,), (0,)), ((), ())), preferred_element_type=jnp.float32
    )
    twice_applied = matmul(
        gram_cols.T, lax.all_gather(applied.astype(jnp.bfloat16), "tp", axis=0, tiled=True)
    )
    mixed = (
        quintic_one * grad_iterate.astype(jnp.float32)
        + quintic_three * applied
        + quintic_five * twice_applied
    )
    return mixed * math.sqrt(C)


def chunks_of(width):
    for count in (3, 2):
        if width % (count * 128) == 0:
            return count
    return 1


def paired(devices, own):
    rows, width = own.shape
    half = rows // 2
    piece = rows // (2 * devices)
    swap = [(0, 1), (1, 0)]
    first = lax.axis_index("tp") == 0

    def reduced(partial):
        share = lax.psum_scatter(partial, "fsdp", scatter_dimension=0, tiled=True)
        return share.astype(jnp.bfloat16)

    other = lax.ppermute(own, "tp", swap)

    left_share = reduced(rows_by_rows(own, own[:half]))
    corner_share = reduced(rows_by_rows(own[half:], own[half:]))

    picked = jnp.where(
        first,
        other.reshape(devices, 2, piece, width)[:, 0],
        own.reshape(devices, 2, piece, width)[:, 1],
    ).reshape(half, width)
    cross_share = reduced(rows_by_rows(picked, jnp.where(first, own, other)))
    cross_share = lax.all_gather(cross_share, "tp", axis=0, tiled=True)

    left = lax.all_gather(left_share, "fsdp", axis=0, tiled=True)
    corner = lax.all_gather(corner_share, "fsdp", axis=0, tiled=True)
    diagonal = jnp.concatenate(
        [left, jnp.concatenate([left[half:].T, corner], axis=0)], axis=1
    )
    cross = lax.all_gather(cross_share, "fsdp", axis=0, tiled=True)
    cross = jnp.where(first, cross.T, cross)

    count = chunks_of(width)
    step = width // count
    spans = [slice(i * step, (i + 1) * step) for i in range(count)]
    applied = [matmul(diagonal, own[:, s]) + matmul(cross, other[:, s]) for s in spans]
    low = [a.astype(jnp.bfloat16) for a in applied]
    far = [lax.ppermute(a, "tp", swap) for a in low]
    near = [matmul(diagonal, a) for a in low]
    out = []
    for i, s in enumerate(spans):
        twice = near[i] + matmul(cross, far[i])
        mixed = (
            quintic_one * own[:, s].astype(jnp.float32)
            + quintic_three * applied[i]
            + quintic_five * twice
        )
        out.append(mixed * math.sqrt(C))
    return jnp.concatenate(out, axis=1)


def solution(mesh):
    devices = mesh.shape["fsdp"]
    pair = mesh.shape["tp"] == 2

    def local(grad_iterate):
        if pair and grad_iterate.shape[0] % (2 * devices) == 0:
            return paired(devices, grad_iterate)
        return general(grad_iterate)

    return jax.shard_map(
        local,
        mesh=mesh,
        in_specs=(P("tp", "fsdp"),),
        out_specs=P("tp", "fsdp"),
        check_vma=False,
    )
```
